256 devices in a mesh: row: 8 (over z), col: 32 (over y, x, core).
Axes of the slice: x: 4, y: 4, z: 8, core: 2. Of those that a mesh axis runs over, the one named last changes fastest.
Arguments:
- factor: bfloat16 [131072, 5, 1024], P('col', None, 'row'), may hold values from -0.0625 to 0.0625
- diag_inverse: bfloat16 [5, 1024, 1024], P(None, 'row'), may hold values from -1 to 2
- right_side: float32 [16, 128, 1024], P(None, 'col', 'row'), may hold values from -6 to 6
- tile_order: int32 [128], replicated, may hold values from 0 to 127, each once
- live_segments: int32 [16], replicated, may hold values from 2 to 5
Outputs:
- result: float32 [16, 128, 1024], P(None, 'col', 'row')
The draws below stay inside these ranges and needn't reach their ends.
Inputs may be any that keep to these rules, and one draw needn't show every extreme that they name: `tile_order`: each of 0 to 127 appears once.
All inputs are finite; a program needn't handle non-finite values.
Results may differ from the reference program's by a relative error of at most 0.0019.
Values may be sent and summed in bfloat16 or wider, within the bound.
No kernel may reach another device: no remote copies, remote signals or barrier semaphores. Data moves between devices by JAX's collectives and lax.ppermute only.
A program may use at most 64 MiB of HBM per device.

```python
import math
import jax
import jax.numpy as jnp
from jax import lax

TB = 1024
NRHS = 16
SECTIONS = 5
K = 128
N = 131072


def draw_diag_inverse(key, part):
    identity = jnp.broadcast_to(jnp.eye(TB, dtype=jnp.float32), (SECTIONS, TB, TB))
    noise = jax.random.normal(key, (SECTIONS, TB, TB), jnp.float32) * (0.4 / math.sqrt(TB))
    return (identity + noise).astype(jnp.bfloat16)


def place_ends(values, stream_key, low, top_value):
    shape = values.shape
    place = [jax.random.randint(jax.random.fold_in(stream_key, axis), (), 0, shape[axis]) for axis in range(len(shape))]
    values = values.at[tuple(place)].set(low)
    longest = shape.index(max(shape))
    place[longest] = (place[longest] + 1) % shape[longest]
    return values.at[tuple(place)].set(top_value)


def level_of(own_key, shape, cuts, least, high):
    gain = 1.0
    for position, blocks in cuts:
        heights = jax.random.uniform(jax.random.fold_in(jax.random.fold_in(own_key, 6), position), (blocks,), jnp.float32, least / len(cuts), high / len(cuts))
        gain = gain * jnp.repeat(jnp.exp(heights), shape[position] // blocks).reshape((-1,) + (1,) * (len(shape) - 1 - position))
    return gain


def scatter_about(rng, extent, scale, limit, cuts=(), kind=jnp.bfloat16):
    loudness = level_of(rng, extent, cuts, -0.22, 0.18) if cuts else 1.0
    entries = jax.random.normal(rng, extent, jnp.float32) * scale * loudness
    return jnp.minimum(jnp.maximum(entries, -limit), limit).astype(kind)


def setup_inputs(seed: int = 0) -> dict:
    key_of = jax.random.split(jax.random.key(seed), 6)
    factor = scatter_about(key_of[0], (N, SECTIONS, TB), (2 * SECTIONS * TB) ** -0.5, 0.0625, ((0, 32), (2, 8)))
    diag_inverse = draw_diag_inverse(jax.random.fold_in(key_of[5], 71), 0)
    right_side = scatter_about(key_of[2], (NRHS, K, TB), 1.0, 6.0, ((1, 32), (2, 8)), jnp.float32)
    tile_order = jax.random.permutation(key_of[3], K).astype(jnp.int32)
    live_segments = place_ends(jax.random.randint(key_of[4], (NRHS,), SECTIONS // 2, SECTIONS + 1), jax.random.fold_in(key_of[4], 1), SECTIONS // 2, SECTIONS).astype(jnp.int32)
    return dict(factor=factor, diag_inverse=diag_inverse, right_side=right_side, tile_order=tile_order, live_segments=live_segments)


def reference(factor, diag_inverse, right_side, tile_order, live_segments):
    segment_limit = live_segments.astype(jnp.int32)
    partial_value = jnp.zeros((NRHS, K * TB), jnp.float32)
    result = jnp.zeros((NRHS, K, TB), jnp.float32)
    for section in range(SECTIONS):
        slot_id = tile_order[section].astype(jnp.int32)
        offset = (slot_id * TB).astype(jnp.int32)
        rhs_tile = lax.dynamic_index_in_dim(right_side, slot_id, 1, keepdims=False)
        remaining = rhs_tile - lax.dynamic_slice_in_dim(partial_value, offset, TB, 1)
        inverse = diag_inverse[section].astype(jnp.float32)
        solved = lax.dot_general(remaining, inverse, (((1,), (1,)), ((), ())),
                                 precision=lax.Precision.HIGHEST, preferred_element_type=jnp.float32)
        is_live = (section < segment_limit)[:, None]
        sent_block = jnp.where(is_live, solved, jnp.zeros_like(solved)).astype(jnp.bfloat16)
        partial_value = partial_value + lax.dot_general(sent_block, factor[:, section, :], (((1,), (1,)), ((), ())),
                                            preferred_element_type=jnp.float32)
        stored = jnp.where(is_live, solved, remaining)
        result = lax.dynamic_update_slice_in_dim(result, stored[:, None, :], slot_id, 1)
    slot_ids = jnp.arange(K, dtype=jnp.int32)
    visited = jnp.any(slot_ids[:, None] == tile_order[:SECTIONS][None, :], axis=1)
    trailing = right_side - partial_value.reshape(NRHS, K, TB)
    return jnp.where(visited[None, :, None], result, trailing)
```

```python
import jax
import jax.numpy as jnp
from jax import lax
from jax.sharding import PartitionSpec as P


def sent_to_all(array, axis):
    peers = lax.axis_size(axis)
    return lax.all_to_all(
        jnp.broadcast_to(array[None], (peers, *array.shape)), axis, 0, 0, tiled=True
    )


def moved_by_mask(array, axis, mask):
    size = lax.axis_size(axis)

    def by(fixed):
        if fixed == 0:
            return lambda value: value
        pairs = [(i, i ^ fixed) for i in range(size)]
        return lambda value: lax.ppermute(value, axis, pairs)

    return lax.switch(mask, [by(fixed) for fixed in range(size)], array)


def per_device(factor, diag_inverse, right_side, tile_order, live_segments):
    section_count, slice_width, tile_width = diag_inverse.shape
    rhs_count, rows_dev, _ = right_side.shape
    row_size = tile_width // slice_width
    my_col = lax.axis_index("col")
    slots = tile_order[:section_count]
    owner = lax.div(slots, jnp.int32(rows_dev))
    place = lax.rem(slots, jnp.int32(rows_dev))
    masks = owner[1:] ^ owner[:-1]
    local = jnp.arange(rows_dev, dtype=jnp.int32)
    whole = sent_to_all(right_side, "row")
    history = None
    result = jnp.zeros_like(right_side)
    for section in range(section_count):
        here = local == place[section]
        tile = jnp.where(here[None, None, :, None], whole, 0.0).sum(axis=2)
        remaining = jnp.moveaxis(tile, 0, 1).reshape(rhs_count, tile_width)
        if section:
            rows = lax.dynamic_slice_in_dim(factor, place[section] * tile_width, tile_width, 0)
            part = jnp.zeros((rhs_count, tile_width), jnp.float32)
            for before in range(section):
                part = part + lax.dot_general(
                    history[before], rows[:, before, :], (((1,), (1,)), ((), ())),
                    preferred_element_type=jnp.float32,
                )
            arrived = sent_to_all(part.astype(jnp.bfloat16), "row")
            remaining = remaining - arrived.astype(jnp.float32).sum(axis=0)
        solved = lax.dot_general(
            remaining,
            diag_inverse[section].astype(jnp.float32),
            (((1,), (1,)), ((), ())),
            precision=lax.Precision.HIGHEST,
            preferred_element_type=jnp.float32,
        )
        is_live = (section < live_segments)[:, None]
        mine = (here & (my_col == owner[section]))[None, :, None] & is_live[:, :, None]
        result = jnp.where(mine, solved[:, None, :], result)
        sent = jnp.where(is_live, solved, 0.0).astype(jnp.bfloat16)[None]
        history = sent if history is None else jnp.concatenate([history, sent])
        if section < section_count - 1:
            history = moved_by_mask(history, "col", masks[section])
    everywhere = sent_to_all(history, "col")
    history = lax.dynamic_index_in_dim(everywhere, owner[-1], 0, keepdims=False)
    part = jnp.zeros((rhs_count, rows_dev * tile_width), jnp.float32)
    for section in range(section_count):
        part = part + lax.dot_general(
            history[section], factor[:, section, :], (((1,), (1,)), ((), ())),
            preferred_element_type=jnp.float32,
        )
    pieces = part.astype(jnp.bfloat16).reshape(rhs_count, rows_dev, row_size, slice_width)
    pieces = jnp.moveaxis(pieces, 2, 0)
    total = lax.all_to_all(pieces, "row", 0, 0, tiled=True).astype(jnp.float32).sum(axis=0)
    order = jnp.arange(section_count, dtype=jnp.int32)
    slot_here = my_col * rows_dev + local
    solved_here = (slot_here[None, :, None] == slots[:, None, None]) & (
        order[:, None, None] < live_segments[None, None, :]
    )
    done = solved_here.any(axis=0).T[:, :, None]
    return jnp.where(done, result, right_side - total)


def solution(mesh):
    return jax.shard_map(
        per_device,
        mesh=mesh,
        in_specs=(P("col", None, "row"), P(None, "row", None), P(None, "col", "row"), P(), P()),
        out_specs=P(None, "col", "row"),
        check_vma=False,
    )
```

```python
import functools

import jax
import jax.numpy as jnp
from jax import lax
from jax.experimental import pallas as pl
from jax.experimental.pallas import tpu as pltpu
from jax.sharding import PartitionSpec as P


NT = (((1,), (1,)), ((), ()))


def sent_to_all(array, axis):
    peers = lax.axis_size(axis)
    return lax.all_to_all(
        jnp.broadcast_to(array[None], (peers, *array.shape)), axis, 0, 0, tiled=True
    )


def levels(size):
    bits = size.bit_length() - 1
    cuts, low = [(0, 1)], 1
    while low < bits:
        cuts.append((low, min(2, bits - low)))
        low += 2
    return cuts[::-1]


def from_mask(array, mask):
    size = lax.axis_size("col")
    return lax.ppermute(array, "col", [(i, i ^ mask) for i in range(size)])


def moved_by_mask(array, mask):
    for low, bits in levels(lax.axis_size("col")):
        part = lax.shift_right_logical(mask, jnp.int32(low)) & ((1 << bits) - 1)
        branches = [lambda value: value]
        for step in range(1, 1 << bits):
            branches.append(functools.partial(from_mask, mask=step << low))
        array = lax.switch(part, branches, array)
    return array


def spread(array, owner):
    away = lax.axis_index("col") ^ owner
    for low, bits in levels(lax.axis_size("col")):
        part = lax.shift_right_logical(away, jnp.int32(low)) & ((1 << bits) - 1)
        arrived = [from_mask(array, step << low) for step in range(1, 1 << bits)]
        for step, other in enumerate(arrived, 1):
            array = jnp.where(part == step, other, array)
    return array


def partial_kernel(place_ref, sent_ref, rows_ref, out_ref):
    total = lax.dot_general(sent_ref[0], rows_ref[0], NT, preferred_element_type=jnp.float32)
    for before in range(1, sent_ref.shape[0]):
        total = total + lax.dot_general(
            sent_ref[before], rows_ref[before], NT, preferred_element_type=jnp.float32
        )
    rounded = total.astype(out_ref.dtype)
    for peer in range(out_ref.shape[0]):
        out_ref[peer] = rounded


def partial_for_all(sent, factor, place, tile_width, peers):
    count, rhs_count, width = sent.shape
    return pl.pallas_call(
        partial_kernel,
        out_shape=jax.ShapeDtypeStruct((peers, rhs_count, tile_width), jnp.bfloat16),
        grid_spec=pltpu.PrefetchScalarGridSpec(
            num_scalar_prefetch=1,
            grid=(1,),
            in_specs=[
                pl.BlockSpec((count, rhs_count, width), lambda i, place: (0, 0, 0)),
                pl.BlockSpec((count, tile_width, width), lambda i, place: (0, place[0], 0)),
            ],
            out_specs=pl.BlockSpec((peers, rhs_count, tile_width), lambda i, place: (0, 0, 0)),
        ),
        cost_estimate=pl.CostEstimate(
            flops=2 * count * rhs_count * width * tile_width,
            bytes_accessed=2 * count * width * tile_width,
            transcendentals=0,
        ),
    )(place[None], sent, factor)


def trailing_kernel(sent_ref, rows_ref, out_ref):
    total = lax.dot_general(sent_ref[0], rows_ref[0], NT, preferred_element_type=jnp.float32)
    for before in range(1, sent_ref.shape[0]):
        total = total + lax.dot_general(
            sent_ref[before], rows_ref[before], NT, preferred_element_type=jnp.float32
        )
    rounded = total.astype(out_ref.dtype)
    width = out_ref.shape[3]
    for peer in range(out_ref.shape[0]):
        out_ref[peer, 0] = rounded[:, peer * width : (peer + 1) * width]


def trailing(sent, factor, tile_width, peers):
    count, rhs_count, width = sent.shape
    tiles = factor.shape[1] // tile_width
    return pl.pallas_call(
        trailing_kernel,
        out_shape=jax.ShapeDtypeStruct((peers, tiles, rhs_count, width), jnp.bfloat16),
        grid=(tiles,),
        in_specs=[
            pl.BlockSpec((count, rhs_count, width), lambda i: (0, 0, 0)),
            pl.BlockSpec((count, tile_width, width), lambda i: (0, i, 0)),
        ],
        out_specs=pl.BlockSpec((peers, 1, rhs_count, width), lambda i: (0, i, 0, 0)),
        cost_estimate=pl.CostEstimate(
            flops=2 * count * rhs_count * width * tile_width * tiles,
            bytes_accessed=2 * count * width * tile_width * tiles,
            transcendentals=0,
        ),
    )(sent, factor)


def per_device(factor, diag_inverse, right_side, tile_order, live_segments):
    section_count, slice_width, tile_width = diag_inverse.shape
    rhs_count, rows_dev, _ = right_side.shape
    peers = tile_width // slice_width
    my_col = lax.axis_index("col")
    factor = jnp.transpose(factor, (1, 0, 2))
    slots = tile_order[:section_count]
    owner = lax.div(slots, jnp.int32(rows_dev))
    place = lax.rem(slots, jnp.int32(rows_dev))
    masks = owner[1:] ^ owner[:-1]
    local = jnp.arange(rows_dev, dtype=jnp.int32)
    whole = sent_to_all(right_side, "row")
    history = None
    result = jnp.zeros_like(right_side)
    for section in range(section_count):
        here = local == place[section]
        tile = jnp.where(here[None, None, :, None], whole, 0.0).sum(axis=2)
        remaining = jnp.moveaxis(tile, 0, 1).reshape(rhs_count, tile_width)
        if section:
            parts = partial_for_all(history, factor, place[section], tile_width, peers)
            arrived = lax.all_to_all(parts, "row", 0, 0, tiled=True)
            remaining = remaining - arrived.astype(jnp.float32).sum(axis=0)
        solved = lax.dot_general(
            remaining,
            diag_inverse[section].astype(jnp.float32),
            NT,
            precision=lax.Precision.HIGHEST,
            preferred_element_type=jnp.float32,
        )
        is_live = (section < live_segments)[:, None]
        mine = (here & (my_col == owner[section]))[None, :, None] & is_live[:, :, None]
        result = jnp.where(mine, solved[:, None, :], result)
        sent = jnp.where(is_live, solved, 0.0).astype(jnp.bfloat16)[None]
        history = sent if history is None else jnp.concatenate([history, sent])
        if section < section_count - 1:
            history = moved_by_mask(history, masks[section])
    history = spread(history, owner[-1])
    pieces = trailing(history, factor, tile_width, peers)
    arrived = lax.all_to_all(pieces, "row", 0, 0, tiled=True)
    total = jnp.moveaxis(arrived.astype(jnp.float32).sum(axis=0), 0, 1)
    order = jnp.arange(section_count, dtype=jnp.int32)
    slot_here = my_col * rows_dev + local
    solved_here = (slot_here[None, :, None] == slots[:, None, None]) & (
        order[:, None, None] < live_segments[None, None, :]
    )
    done = solved_here.any(axis=0).T[:, :, None]
    return jnp.where(done, result, right_side - total)


def solution(mesh):
    return jax.shard_map(
        per_device,
        mesh=mesh,
        in_specs=(P("col", None, "row"), P(None, "row", None), P(None, "col", "row"), P(), P()),
        out_specs=P(None, "col", "row"),
        check_vma=False,
    )
```

```python
import functools

import jax
import jax.numpy as jnp
from jax import lax
from jax.experimental import pallas as pl
from jax.experimental.pallas import tpu as pltpu
from jax.sharding import PartitionSpec as P

NT = (((1,), (1,)), ((), ()))
F32 = jnp.float32
BF16 = jnp.bfloat16


def to_all(array, axis, peers, groups=None):
    copies = jnp.broadcast_to(array[None], (peers, *array.shape))
    return lax.all_to_all(copies, axis, 0, 0, axis_index_groups=groups, tiled=True)


def pair_groups(rows, cols, mask):
    firsts = [c for c in range(cols) if c <= c ^ mask]
    return [
        [r * cols + c for c in dict.fromkeys((first, first ^ mask)) for r in range(rows)]
        for first in firsts
    ]


def gathered_at_pair(array, source, target):
    rows, cols = lax.axis_size("row"), lax.axis_size("col")

    def by(mask, value):
        groups = pair_groups(rows, cols, mask)
        arrived = to_all(value, ("row", "col"), len(groups[0]), groups)
        return arrived if mask else jnp.concatenate([arrived, arrived])

    branches = [functools.partial(by, mask) for mask in range(cols)]
    return lax.switch(source ^ target, branches, array)


def split(value):
    high = value.astype(BF16)
    rest = value - high.astype(F32)
    middle = rest.astype(BF16)
    low = (rest - middle.astype(F32)).astype(BF16)
    return [high, middle, low]


def step_kernel(at_ref, arrived_ref, inverse_ref, live_ref, rows_ref, solved_ref, sent_ref, pieces_ref):
    section, me = at_ref[0], at_ref[1]
    peers, _, rhs_count, width = arrived_ref.shape
    total = jnp.zeros((3 * rhs_count, width), F32)
    for peer in range(peers):
        parts = jnp.concatenate([arrived_ref[peer, k] for k in range(3)], axis=0)
        inverse = inverse_ref[0, :, peer * width : (peer + 1) * width]
        total = total + lax.dot_general(parts, inverse, NT, preferred_element_type=F32)
    solved = total[:rhs_count] + total[rhs_count : 2 * rhs_count] + total[2 * rhs_count :]
    solved_ref[...] = solved
    sent = jnp.where(live_ref[0] > 0, solved, 0.0).astype(BF16)
    slots = sent_ref.shape[0]
    part = None
    for slot in range(slots):
        older = arrived_ref[me, 3 + slot] if slot < slots - 1 else jnp.zeros_like(sent)
        value = jnp.where(section == slot, sent, older)
        sent_ref[slot] = value
        term = lax.dot_general(value, rows_ref[slot], NT, preferred_element_type=F32)
        part = term if part is None else part + term
    for peer in range(peers):
        pieces_ref[peer] = part[:, peer * width : (peer + 1) * width]


def step(arrived, diag_inverse, live, factor, section, me, place, half):
    both, count, rhs_count, width = arrived.shape
    peers = both // 2
    tile_width = diag_inverse.shape[2]
    slots = count - 2
    return pl.pallas_call(
        step_kernel,
        out_shape=(
            jax.ShapeDtypeStruct((rhs_count, width), F32),
            jax.ShapeDtypeStruct((slots, rhs_count, width), BF16),
            jax.ShapeDtypeStruct((peers, rhs_count, width), F32),
        ),
        grid_spec=pltpu.PrefetchScalarGridSpec(
            num_scalar_prefetch=1,
            grid=(1,),
            in_specs=[
                pl.BlockSpec((peers, count, rhs_count, width), lambda i, at: (at[3], 0, 0, 0)),
                pl.BlockSpec((1, width, tile_width), lambda i, at: (at[0], 0, 0)),
                pl.BlockSpec((1, rhs_count, width), lambda i, at: (at[0], 0, 0)),
                pl.BlockSpec((slots, tile_width, width), lambda i, at: (0, at[2], 0)),
            ],
            out_specs=[
                pl.BlockSpec((rhs_count, width), lambda i, at: (0, 0)),
                pl.BlockSpec((slots, rhs_count, width), lambda i, at: (0, 0, 0)),
                pl.BlockSpec((peers, rhs_count, width), lambda i, at: (0, 0, 0)),
            ],
        ),
        compiler_params=pltpu.CompilerParams(vmem_limit_bytes=8 << 20),
        cost_estimate=pl.CostEstimate(
            flops=2 * slots * rhs_count * width * tile_width,
            bytes_accessed=2 * slots * width * tile_width,
            transcendentals=0,
        ),
    )(jnp.stack([section, me, place, half]), arrived, diag_inverse, live, factor)


def trailing_kernel(sent_ref, rows_ref, out_ref):
    total = lax.dot_general(sent_ref[0], rows_ref[0], NT, preferred_element_type=F32)
    for before in range(1, sent_ref.shape[0]):
        total = total + lax.dot_general(
            sent_ref[before], rows_ref[before], NT, preferred_element_type=F32
        )
    width = out_ref.shape[3]
    for peer in range(out_ref.shape[0]):
        out_ref[peer, 0] = total[:, peer * width : (peer + 1) * width]


def trailing(sent, factor, tile_width, peers):
    count, rhs_count, width = sent.shape
    tiles = factor.shape[1] // tile_width
    return pl.pallas_call(
        trailing_kernel,
        out_shape=jax.ShapeDtypeStruct((peers, tiles, rhs_count, width), F32),
        grid=(tiles,),
        in_specs=[
            pl.BlockSpec((count, rhs_count, width), lambda i: (0, 0, 0)),
            pl.BlockSpec((count, tile_width, width), lambda i: (0, i, 0)),
        ],
        out_specs=pl.BlockSpec((peers, 1, rhs_count, width), lambda i: (0, i, 0, 0)),
        compiler_params=pltpu.CompilerParams(vmem_limit_bytes=12 << 20),
        cost_estimate=pl.CostEstimate(
            flops=2 * count * rhs_count * width * tile_width * tiles,
            bytes_accessed=2 * count * width * tile_width * tiles,
            transcendentals=0,
        ),
    )(sent, factor)


def per_device(factor, diag_inverse, right_side, tile_order, live_segments):
    section_count, slice_width, tile_width = diag_inverse.shape
    rhs_count, rows_dev, _ = right_side.shape
    peers = tile_width // slice_width
    last = section_count - 1
    my_col, me = lax.axis_index("col"), lax.axis_index("row")
    factor = jnp.transpose(factor, (1, 0, 2))
    slots = tile_order[:section_count]
    owner = lax.div(slots, jnp.int32(rows_dev))
    place = lax.rem(slots, jnp.int32(rows_dev))
    local = jnp.arange(rows_dev, dtype=jnp.int32)
    order = jnp.arange(section_count, dtype=jnp.int32)
    live = (order[:, None] < live_segments[None, :]).astype(F32)
    live = jnp.broadcast_to(live[:, :, None], (section_count, rhs_count, slice_width))
    here = place[:, None] == local[None, :]
    sides = jnp.where(here[:, None, :, None], right_side[None], 0.0).sum(axis=2)
    history = jnp.zeros((last, rhs_count, slice_width), BF16)
    solves = jnp.zeros((section_count, rhs_count, slice_width), F32)

    def one(section, carry):
        side, history, solves = carry
        source, target = owner[section], owner[section + 1]
        carried = jnp.stack([*split(side), *[history[k] for k in range(last - 1)]])
        involved = (my_col == source) | (my_col == target)
        arrived = lax.cond(
            involved,
            lambda value: gathered_at_pair(value, source, target),
            lambda value: jnp.zeros((2 * peers, *value.shape), value.dtype),
            carried,
        )
        solved, history, pieces = step(
            arrived,
            diag_inverse,
            live,
            factor,
            jnp.int32(section),
            me,
            place[section + 1],
            (source > target).astype(jnp.int32),
        )
        solves = jnp.where((order == section)[:, None, None], solved[None], solves)
        side = lax.dynamic_index_in_dim(sides, section + 1, 0, keepdims=False)
        pieces, history, solves, side = lax.optimization_barrier((pieces, history, solves, side))
        total = lax.all_to_all(pieces, "row", 0, 0, tiled=True).sum(axis=0)
        return side - total, history, solves

    side, history, solves = lax.fori_loop(0, last, one, (sides[0], history, solves))
    mine = here & (owner == my_col)[:, None]
    taken = mine[:, None, :, None] & (live > 0)[:, :, None, :]
    done = taken.any(axis=0)
    side, done, taken = lax.optimization_barrier((side, done, taken))
    remaining = jnp.moveaxis(to_all(side, "row", peers), 0, 1).reshape(rhs_count, tile_width)
    solved = lax.dot_general(
        remaining,
        diag_inverse[last].astype(F32),
        NT,
        precision=lax.Precision.HIGHEST,
        preferred_element_type=F32,
    )
    solves = jnp.where((order == last)[:, None, None], solved[None], solves)
    result = jnp.where(taken, solves[:, :, None, :], 0.0).sum(axis=0)
    sent = jnp.where(live[last] > 0, solved, 0.0).astype(BF16)
    history = jnp.concatenate([history, sent[None]])
    history, result = lax.optimization_barrier((history, result))
    everywhere = to_all(history, "col", lax.axis_size("col"))
    history = lax.dynamic_index_in_dim(everywhere, owner[last], 0, keepdims=False)
    pieces = trailing(history, factor, tile_width, peers)
    total = lax.all_to_all(pieces, "row", 0, 0, tiled=True).sum(axis=0)
    updated = right_side - jnp.moveaxis(total, 0, 1)
    return jnp.where(done, result, updated)


def solution(mesh):
    return jax.shard_map(
        per_device,
        mesh=mesh,
        in_specs=(P("col", None, "row"), P(None, "row", None), P(None, "col", "row"), P(), P()),
        out_specs=P(None, "col", "row"),
        check_vma=False,
    )
```

```python
import functools

import jax
import jax.numpy as jnp
from jax import lax
from jax.experimental import pallas as pl
from jax.experimental.pallas import tpu as pltpu
from jax.sharding import PartitionSpec as P

NT = (((1,), (1,)), ((), ()))
F32 = jnp.float32
BF16 = jnp.bfloat16


def to_all(array, axis, peers, groups=None):
    copies = jnp.broadcast_to(array[None], (peers, *array.shape))
    return lax.all_to_all(copies, axis, 0, 0, axis_index_groups=groups, tiled=True)


def from_mask(array, mask):
    size = lax.axis_size("col")
    return lax.ppermute(array, "col", [(i, i ^ mask) for i in range(size)])


def levels(size):
    bits = size.bit_length() - 1
    return [(low, min(2, bits - low)) for low in range(1, bits, 2)][::-1]


def moved_by_mask(array, parts):
    for (low, bits), part in zip(levels(lax.axis_size("col")), parts, strict=True):
        branches = [lambda value: value]
        for step in range(1, 1 << bits):
            branches.append(functools.partial(from_mask, mask=step << low))
        array = lax.switch(part, branches, array)
    return array


def partial_kernel(section, at_ref, sent_ref, rows_ref, side_ref, keep_ref, give_ref):
    me, core = at_ref[0], at_ref[1]
    total = lax.dot_general(sent_ref[0], rows_ref[0], NT, preferred_element_type=F32)
    for before in range(1, section):
        total = total + lax.dot_general(
            sent_ref[before], rows_ref[before], NT, preferred_element_type=F32
        )
    half, width = keep_ref.shape[0], side_ref.shape[2]
    columns = pl.ds(pl.multiple_of(me * width, width), width)
    for out_ref, first in ((keep_ref, core == 0), (give_ref, core != 0)):
        out_ref[...] = -jnp.where(first, total[:half], total[half:])
        side = jnp.where(first, side_ref[0, :half], side_ref[0, half:])
        out_ref[:, columns] = out_ref[:, columns] + side


def partial_halves(section, at, sent, factor, sides, tile_width):
    _, rhs_count, width = sent.shape
    half = rhs_count // 2
    return pl.pallas_call(
        functools.partial(partial_kernel, section),
        out_shape=[jax.ShapeDtypeStruct((half, tile_width), F32)] * 2,
        grid_spec=pltpu.PrefetchScalarGridSpec(
            num_scalar_prefetch=1,
            grid=(1,),
            in_specs=[
                pl.BlockSpec((section, rhs_count, width), lambda i, at: (0, 0, 0)),
                pl.BlockSpec((section, tile_width, width), lambda i, at: (0, at[2 + section], 0)),
                pl.BlockSpec((1, rhs_count, width), lambda i, at: (section, 0, 0)),
            ],
            out_specs=[pl.BlockSpec((half, tile_width), lambda i, at: (0, 0))] * 2,
        ),
        compiler_params=pltpu.CompilerParams(vmem_limit_bytes=6 << 20),
        cost_estimate=pl.CostEstimate(
            flops=2 * section * rhs_count * width * tile_width,
            bytes_accessed=2 * section * width * tile_width,
            transcendentals=0,
        ),
    )(at, sent, factor, sides)


def trailing_kernel(sent_ref, rows_ref, out_ref):
    total = lax.dot_general(sent_ref[0], rows_ref[0], NT, preferred_element_type=F32)
    for before in range(1, sent_ref.shape[0]):
        total = total + lax.dot_general(
            sent_ref[before], rows_ref[before], NT, preferred_element_type=F32
        )
    width = out_ref.shape[3]
    for peer in range(out_ref.shape[0]):
        out_ref[peer, 0] = total[:, peer * width : (peer + 1) * width]


def trailing(sent, factor, tile_width, peers):
    count, rhs_count, width = sent.shape
    tiles = factor.shape[1] // tile_width
    return pl.pallas_call(
        trailing_kernel,
        out_shape=jax.ShapeDtypeStruct((peers, tiles, rhs_count, width), F32),
        grid=(tiles,),
        in_specs=[
            pl.BlockSpec((count, rhs_count, width), lambda i: (0, 0, 0)),
            pl.BlockSpec((count, tile_width, width), lambda i: (0, i, 0)),
        ],
        out_specs=pl.BlockSpec((peers, 1, rhs_count, width), lambda i: (0, i, 0, 0)),
        compiler_params=pltpu.CompilerParams(vmem_limit_bytes=10 << 20),
        cost_estimate=pl.CostEstimate(
            flops=2 * count * rhs_count * width * tile_width * tiles,
            bytes_accessed=2 * count * width * tile_width * tiles,
            transcendentals=0,
        ),
    )(sent, factor)


def per_device(factor, diag_inverse, right_side, tile_order, live_segments):
    section_count, slice_width, tile_width = diag_inverse.shape
    rhs_count, rows_dev, _ = right_side.shape
    half = rhs_count // 2
    peers = tile_width // slice_width
    cols = lax.axis_size("col")
    my_col, me = lax.axis_index("col"), lax.axis_index("row")
    core = my_col & 1
    factor = jnp.transpose(factor, (1, 0, 2))
    slots = tile_order[:section_count]
    owner = lax.div(slots, jnp.int32(rows_dev))
    place = lax.rem(slots, jnp.int32(rows_dev))
    local = jnp.arange(rows_dev, dtype=jnp.int32)
    order = jnp.arange(section_count, dtype=jnp.int32)
    here = place[:, None] == local[None, :]
    sides = jnp.where(here[:, None, :, None], right_side[None], 0.0).sum(axis=2)
    mine = owner == my_col

    def halves_of(array):
        low, high = array[:half], array[half:]
        return jnp.where(core == 0, low, high), jnp.where(core == 0, high, low)

    keep, give = halves_of(sides[0])
    slice_of_half = jnp.where(mine[0], keep, from_mask(give, 1))
    arrived = to_all(slice_of_half, "row", peers)

    masks = owner[1:] ^ owner[:-1]
    parts = [
        lax.shift_right_logical(masks, jnp.int32(low)) & ((1 << bits) - 1)
        for low, bits in levels(cols)
    ]
    at = jnp.concatenate([jnp.stack([me, core]), place]).astype(jnp.int32)
    live = order[:, None] < live_segments[None, :]
    taken = (here & mine[:, None])[:, None, :] & live[:, :, None]
    done = taken.any(axis=0)[:, :, None]
    arrived, parts, at, live, taken, done, mine, sides = lax.optimization_barrier(
        (arrived, parts, at, live, taken, done, mine, sides)
    )

    remaining = jnp.moveaxis(arrived, 0, 1).reshape(half, tile_width)
    history = None
    solves = []
    for section in range(section_count):
        if section:
            keep, give = partial_halves(section, at, history, factor, sides, tile_width)
            share = jnp.where(mine[section], keep, from_mask(give, 1))
            remaining = to_all(share, "row", peers).sum(axis=0)
        solved = lax.dot_general(
            remaining,
            diag_inverse[section].astype(F32),
            NT,
            precision=lax.Precision.HIGHEST,
            preferred_element_type=F32,
        )
        other = from_mask(solved, 1)
        solved = jnp.where(
            core == 0, jnp.concatenate([solved, other]), jnp.concatenate([other, solved])
        )
        solves.append(solved)
        sent = jnp.where(live[section][:, None], solved, 0.0).astype(BF16)[None]
        history = sent if history is None else jnp.concatenate([history, sent])
        if section < section_count - 1:
            history, solves = lax.optimization_barrier((history, solves))
            history = moved_by_mask(history, [part[section] for part in parts])
    result = jnp.where(taken[..., None], jnp.stack(solves)[:, :, None, :], 0.0).sum(axis=0)
    history, result = lax.optimization_barrier((history, result))
    planes = [list(range(first, cols, 2)) for first in range(2)]
    everywhere = to_all(history, "col", cols // 2, planes)
    chip = lax.shift_right_logical(owner[-1], jnp.int32(1))
    history = lax.dynamic_index_in_dim(everywhere, chip, 0, keepdims=False)
    pieces = trailing(history, factor, tile_width, peers)
    total = lax.all_to_all(pieces, "row", 0, 0, tiled=True).sum(axis=0)
    updated = right_side - jnp.moveaxis(total, 0, 1)
    return jnp.where(done, result, updated)


def solution(mesh):
    return jax.shard_map(
        per_device,
        mesh=mesh,
        in_specs=(P("col", None, "row"), P(None, "row", None), P(None, "col", "row"), P(), P()),
        out_specs=P(None, "col", "row"),
        check_vma=False,
    )
```

```python
import functools

import jax
import jax.numpy as jnp
from jax import lax
from jax.experimental import pallas as pl
from jax.experimental.pallas import tpu as pltpu
from jax.sharding import PartitionSpec as P

NT = (((1,), (1,)), ((), ()))
F32 = jnp.float32
BF16 = jnp.bfloat16
CHIP, PLACE, MINE = 2, 3, 8


def to_all(array, axis, peers, groups=None):
    copies = jnp.broadcast_to(array[None], (peers, *array.shape))
    return lax.all_to_all(copies, axis, 0, 0, axis_index_groups=groups, tiled=True)


def from_mask(array, mask):
    size = lax.axis_size("col")
    return lax.ppermute(array, "col", [(i, i ^ mask) for i in range(size)])


def levels(size):
    bits = size.bit_length() - 1
    return [(low, min(2, bits - low)) for low in range(1, bits, 2)][::-1]


def moved_by_mask(array, parts):
    for (low, bits), part in zip(levels(lax.axis_size("col")), parts, strict=True):
        branches = [lambda value: value]
        for step in range(1, 1 << bits):
            branches.append(functools.partial(from_mask, mask=step << low))
        array = lax.switch(part, branches, array)
    return array


def window_kernel(at_ref, *refs):
    count = len(refs) // 2
    for rows_ref, out_ref in zip(refs[:count], refs[count:], strict=True):
        out_ref[...] = rows_ref[...]


def window_rows(at, factor, section_count, tile_width):
    width = factor.shape[2]

    def spec(section, index_map):
        return pl.BlockSpec((section, tile_width, width), index_map)

    later = range(1, section_count)
    return pl.pallas_call(
        window_kernel,
        out_shape=[jax.ShapeDtypeStruct((t, tile_width, width), factor.dtype) for t in later],
        grid_spec=pltpu.PrefetchScalarGridSpec(
            num_scalar_prefetch=1,
            grid=(1,),
            in_specs=[spec(t, lambda i, at, t=t: (0, at[PLACE + t], 0)) for t in later],
            out_specs=[spec(t, lambda i, at: (0, 0, 0)) for t in later],
        ),
        compiler_params=pltpu.CompilerParams(vmem_limit_bytes=14 << 20),
        cost_estimate=pl.CostEstimate(flops=0, bytes_accessed=5 << 20, transcendentals=0),
    )(at, *[factor for _ in later])


def partial_kernel(section, at_ref, sent_ref, own_ref, other_ref, own_side, other_side, out_ref):
    me, core = at_ref[0], at_ref[1]
    peers, half, _ = out_ref.shape
    width = own_side.shape[2]
    columns = pl.ds(pl.multiple_of(me * width, width), width)

    def write(rows_ref, side_ref):
        total = lax.dot_general(sent_ref[0], rows_ref[0], NT, preferred_element_type=F32)
        for before in range(1, section):
            total = total + lax.dot_general(
                sent_ref[before], rows_ref[before], NT, preferred_element_type=F32
            )
        value = -jnp.where(core == 0, total[:half], total[half:])
        side = jnp.where(core == 0, side_ref[0, :half], side_ref[0, half:])
        for peer in range(peers):
            out_ref[peer] = value
            out_ref[peer, :, columns] = out_ref[peer, :, columns] + side

    mine = at_ref[MINE + section]

    @pl.when(mine == 1)
    def _():
        write(own_ref, own_side)

    @pl.when(mine != 1)
    def _():
        write(other_ref, other_side)


def partial_half(section, at, sent, own_rows, other_rows, own_sides, other_sides, peers):
    _, rhs_count, width = sent.shape
    tile_width = own_rows.shape[1]
    half = rhs_count // 2
    rows = pl.BlockSpec((section, tile_width, width), lambda i, at: (0, 0, 0))
    side = pl.BlockSpec((1, rhs_count, width), lambda i, at: (section, 0, 0))
    return pl.pallas_call(
        functools.partial(partial_kernel, section),
        out_shape=jax.ShapeDtypeStruct((peers, half, tile_width), F32),
        grid_spec=pltpu.PrefetchScalarGridSpec(
            num_scalar_prefetch=1,
            grid=(1,),
            in_specs=[
                pl.BlockSpec((section, rhs_count, width), lambda i, at: (0, 0, 0)),
                rows,
                rows,
                side,
                side,
            ],
            out_specs=pl.BlockSpec((peers, half, tile_width), lambda i, at: (0, 0, 0)),
        ),
        compiler_params=pltpu.CompilerParams(vmem_limit_bytes=8 << 20),
        cost_estimate=pl.CostEstimate(
            flops=2 * section * rhs_count * width * tile_width,
            bytes_accessed=4 * section * width * tile_width,
            transcendentals=0,
        ),
    )(at, sent, own_rows, other_rows, own_sides, other_sides)


def trailing_kernel(at_ref, sent_ref, rows_ref, out_ref):
    total = lax.dot_general(sent_ref[0, 0], rows_ref[0], NT, preferred_element_type=F32)
    for before in range(1, rows_ref.shape[0]):
        total = total + lax.dot_general(
            sent_ref[0, before], rows_ref[before], NT, preferred_element_type=F32
        )
    width = out_ref.shape[3]
    for peer in range(out_ref.shape[0]):
        out_ref[peer, 0] = total[:, peer * width : (peer + 1) * width]


def trailing(at, sent, factor, tile_width, peers):
    _, count, rhs_count, width = sent.shape
    tiles = factor.shape[1] // tile_width
    return pl.pallas_call(
        trailing_kernel,
        out_shape=jax.ShapeDtypeStruct((peers, tiles, rhs_count, width), F32),
        grid_spec=pltpu.PrefetchScalarGridSpec(
            num_scalar_prefetch=1,
            grid=(tiles,),
            in_specs=[
                pl.BlockSpec((1, count, rhs_count, width), lambda i, at: (at[CHIP], 0, 0, 0)),
                pl.BlockSpec((count, tile_width, width), lambda i, at: (0, i, 0)),
            ],
            out_specs=pl.BlockSpec((peers, 1, rhs_count, width), lambda i, at: (0, i, 0, 0)),
        ),
        compiler_params=pltpu.CompilerParams(vmem_limit_bytes=10 << 20),
        cost_estimate=pl.CostEstimate(
            flops=2 * count * rhs_count * width * tile_width * tiles,
            bytes_accessed=2 * count * width * tile_width * tiles,
            transcendentals=0,
        ),
    )(at, sent, factor)


def per_device(factor, diag_inverse, right_side, tile_order, live_segments):
    section_count, slice_width, tile_width = diag_inverse.shape
    rhs_count, rows_dev, _ = right_side.shape
    half = rhs_count // 2
    peers = tile_width // slice_width
    cols = lax.axis_size("col")
    my_col, me = lax.axis_index("col"), lax.axis_index("row")
    core = my_col & 1
    factor = jnp.transpose(factor, (1, 0, 2))
    slots = tile_order[:section_count]
    owner = lax.div(slots, jnp.int32(rows_dev))
    place = lax.rem(slots, jnp.int32(rows_dev))
    local = jnp.arange(rows_dev, dtype=jnp.int32)
    order = jnp.arange(section_count, dtype=jnp.int32)
    here = place[:, None] == local[None, :]
    sides = jnp.where(here[:, None, :, None], right_side[None], 0.0).sum(axis=2)
    mine = owner == my_col

    def own_half(array):
        return jnp.where(core == 0, array[:half], array[half:])

    other_sides = from_mask(sides, 1)
    share = own_half(jnp.where(mine[0], sides[0], other_sides[0]))
    arrived = to_all(share, "row", peers)

    chip = lax.shift_right_logical(owner[-1], jnp.int32(1))
    head = jnp.stack([me, core, chip])
    at = jnp.concatenate([head, place, mine.astype(jnp.int32)]).astype(jnp.int32)
    own_rows = window_rows(at, factor, section_count, tile_width)
    other_rows = [from_mask(rows, 1) for rows in own_rows]
    masks = owner[1:] ^ owner[:-1]
    parts = [
        [
            lax.shift_right_logical(masks[section], jnp.int32(low)) & ((1 << bits) - 1)
            for low, bits in levels(cols)
        ]
        for section in range(section_count - 1)
    ]
    live = order[:, None] < live_segments[None, :]
    taken = (here & mine[:, None])[:, None, :] & live[:, :, None]
    done = taken.any(axis=0)[:, :, None]
    first = (arrived, parts, at, live, taken, done, sides, other_sides, own_rows, other_rows)
    arrived, parts, at, live, taken, done, sides, other_sides, own_rows, other_rows = (
        lax.optimization_barrier(first)
    )

    remaining = jnp.moveaxis(arrived, 0, 1).reshape(half, tile_width)
    history = None
    solves = []
    for section in range(section_count):
        if section:
            copies = partial_half(
                section,
                at,
                history,
                own_rows[section - 1],
                other_rows[section - 1],
                sides,
                other_sides,
                peers,
            )
            copies, history, solves = lax.optimization_barrier((copies, history, solves))
            remaining = lax.all_to_all(copies, "row", 0, 0, tiled=True).sum(axis=0)
        solved = lax.dot_general(
            remaining,
            diag_inverse[section].astype(F32),
            NT,
            precision=lax.Precision.HIGHEST,
            preferred_element_type=F32,
        )
        other = from_mask(solved, 1)
        solved = jnp.where(
            core == 0, jnp.concatenate([solved, other]), jnp.concatenate([other, solved])
        )
        solves.append(solved)
        sent = jnp.where(live[section][:, None], solved, 0.0).astype(BF16)[None]
        history = sent if history is None else jnp.concatenate([history, sent])
        if section < section_count - 1:
            history, solves = lax.optimization_barrier((history, solves))
            history = moved_by_mask(history, parts[section])
    result = jnp.where(taken[..., None], jnp.stack(solves)[:, :, None, :], 0.0).sum(axis=0)
    history, result = lax.optimization_barrier((history, result))
    planes = [list(range(first, cols, 2)) for first in range(2)]
    everywhere = to_all(history, "col", cols // 2, planes)
    pieces = trailing(at, everywhere, factor, tile_width, peers)
    total = lax.all_to_all(pieces, "row", 0, 0, tiled=True).sum(axis=0)
    updated = right_side - jnp.moveaxis(total, 0, 1)
    return jnp.where(done, result, updated)


def solution(mesh):
    return jax.shard_map(
        per_device,
        mesh=mesh,
        in_specs=(P("col", None, "row"), P(None, "row", None), P(None, "col", "row"), P(), P()),
        out_specs=P(None, "col", "row"),
        check_vma=False,
    )
```

```python
import functools

import jax
import jax.numpy as jnp
from jax import lax
from jax.experimental import pallas as pl
from jax.experimental.pallas import tpu as pltpu
from jax.sharding import PartitionSpec as P


NT = (((1,), (1,)), ((), ()))
F32 = jnp.float32
BF16 = jnp.bfloat16
CHIP, PLACE, MINE = 2, 3, 8


def to_all(array, axis, peers, groups=None):
    copies = jnp.broadcast_to(array[None], (peers, *array.shape))
    return lax.all_to_all(copies, axis, 0, 0, axis_index_groups=groups, tiled=True)


def from_mask(array, mask):
    size = lax.axis_size("col")
    return lax.ppermute(array, "col", [(i, i ^ mask) for i in range(size)])


def levels(size):
    bits = size.bit_length() - 1
    return [(low, min(2, bits - low)) for low in range(1, bits, 2)][::-1]


def moved_by_mask(array, parts):
    for (low, bits), part in zip(levels(lax.axis_size("col")), parts, strict=True):
        branches = [lambda value: value]
        for step in range(1, 1 << bits):
            branches.append(functools.partial(from_mask, mask=step << low))
        array = lax.switch(part, branches, array)
    return array


def window_kernel(at_ref, *refs):
    count = len(refs) // 2
    for rows_ref, out_ref in zip(refs[:count], refs[count:], strict=True):
        out_ref[...] = rows_ref[...]


def window_rows(at, factor, diag_inverse):
    section_count, width, tile_width = diag_inverse.shape

    def spec(section, index_map):
        return pl.BlockSpec((section, tile_width, width), index_map)

    later = range(1, section_count)
    return pl.pallas_call(
        window_kernel,
        out_shape=[jax.ShapeDtypeStruct((t, tile_width, width), factor.dtype) for t in later]
        + [jax.ShapeDtypeStruct(diag_inverse.shape, diag_inverse.dtype)],
        grid_spec=pltpu.PrefetchScalarGridSpec(
            num_scalar_prefetch=1,
            grid=(1,),
            in_specs=[spec(t, lambda i, at, t=t: (0, at[PLACE + t], 0)) for t in later]
            + [pl.BlockSpec(diag_inverse.shape, lambda i, at: (0, 0, 0))],
            out_specs=[spec(t, lambda i, at: (0, 0, 0)) for t in later]
            + [pl.BlockSpec(diag_inverse.shape, lambda i, at: (0, 0, 0))],
        ),
        compiler_params=pltpu.CompilerParams(vmem_limit_bytes=60 << 20),
        cost_estimate=pl.CostEstimate(flops=0, bytes_accessed=7 << 20, transcendentals=0),
    )(at, *[factor for _ in later], diag_inverse)


def partial_kernel(section, at_ref, sent_ref, own_ref, other_ref, own_side, other_side, out_ref):
    me, core = at_ref[0], at_ref[1]
    peers, half, _ = out_ref.shape
    width = own_side.shape[2]
    columns = pl.ds(pl.multiple_of(me * width, width), width)

    def write(rows_ref, side_ref):
        total = lax.dot_general(sent_ref[0], rows_ref[0], NT, preferred_element_type=F32)
        for before in range(1, section):
            total = total + lax.dot_general(
                sent_ref[before], rows_ref[before], NT, preferred_element_type=F32
            )
        value = -jnp.where(core == 0, total[:half], total[half:])
        side = jnp.where(core == 0, side_ref[0, :half], side_ref[0, half:])
        for peer in range(peers):
            out_ref[peer] = value
            out_ref[peer, :, columns] = out_ref[peer, :, columns] + side

    mine = at_ref[MINE + section]

    @pl.when(mine == 1)
    def _():
        write(own_ref, own_side)

    @pl.when(mine != 1)
    def _():
        write(other_ref, other_side)


def partial_half(section, at, sent, own_rows, other_rows, own_sides, other_sides, peers):
    _, rhs_count, width = sent.shape
    tile_width = own_rows.shape[1]
    half = rhs_count // 2
    rows = pl.BlockSpec((section, tile_width, width), lambda i, at: (0, 0, 0))
    side = pl.BlockSpec((1, rhs_count, width), lambda i, at: (section, 0, 0))
    return pl.pallas_call(
        functools.partial(partial_kernel, section),
        out_shape=jax.ShapeDtypeStruct((peers, half, tile_width), F32),
        grid_spec=pltpu.PrefetchScalarGridSpec(
            num_scalar_prefetch=1,
            grid=(1,),
            in_specs=[
                pl.BlockSpec((section, rhs_count, width), lambda i, at: (0, 0, 0)),
                rows,
                rows,
                side,
                side,
            ],
            out_specs=pl.BlockSpec((peers, half, tile_width), lambda i, at: (0, 0, 0)),
        ),
        compiler_params=pltpu.CompilerParams(vmem_limit_bytes=8 << 20),
        cost_estimate=pl.CostEstimate(
            flops=2 * section * rhs_count * width * tile_width,
            bytes_accessed=4 * section * width * tile_width,
            transcendentals=0,
        ),
    )(at, sent, own_rows, other_rows, own_sides, other_sides)


def trailing_kernel(at_ref, sent_ref, rows_ref, out_ref):
    total = lax.dot_general(sent_ref[0, 0], rows_ref[0], NT, preferred_element_type=F32)
    for before in range(1, rows_ref.shape[0]):
        total = total + lax.dot_general(
            sent_ref[0, before], rows_ref[before], NT, preferred_element_type=F32
        )
    width = out_ref.shape[3]
    for peer in range(out_ref.shape[0]):
        out_ref[peer, 0] = total[:, peer * width : (peer + 1) * width]


def trailing(at, sent, factor, tile_width, peers):
    _, count, rhs_count, width = sent.shape
    tiles = factor.shape[1] // tile_width
    return pl.pallas_call(
        trailing_kernel,
        out_shape=jax.ShapeDtypeStruct((peers, tiles, rhs_count, width), F32),
        grid_spec=pltpu.PrefetchScalarGridSpec(
            num_scalar_prefetch=1,
            grid=(tiles,),
            in_specs=[
                pl.BlockSpec((1, count, rhs_count, width), lambda i, at: (at[CHIP], 0, 0, 0)),
                pl.BlockSpec((count, tile_width, width), lambda i, at: (0, i, 0)),
            ],
            out_specs=pl.BlockSpec((peers, 1, rhs_count, width), lambda i, at: (0, i, 0, 0)),
        ),
        compiler_params=pltpu.CompilerParams(vmem_limit_bytes=60 << 20),
        cost_estimate=pl.CostEstimate(
            flops=2 * count * rhs_count * width * tile_width * tiles,
            bytes_accessed=2 * count * width * tile_width * tiles,
            transcendentals=0,
        ),
    )(at, sent, factor)


def per_device(factor, diag_inverse, right_side, tile_order, live_segments):
    section_count, slice_width, tile_width = diag_inverse.shape
    rhs_count, rows_dev, _ = right_side.shape
    half = rhs_count // 2
    peers = tile_width // slice_width
    cols = lax.axis_size("col")
    my_col, me = lax.axis_index("col"), lax.axis_index("row")
    core = my_col & 1
    factor = jnp.transpose(factor, (1, 0, 2))
    slots = tile_order[:section_count]
    owner = lax.div(slots, jnp.int32(rows_dev))
    place = lax.rem(slots, jnp.int32(rows_dev))
    local = jnp.arange(rows_dev, dtype=jnp.int32)
    order = jnp.arange(section_count, dtype=jnp.int32)
    here = place[:, None] == local[None, :]
    sides = jnp.where(here[:, None, :, None], right_side[None], 0.0).sum(axis=2)
    mine = owner == my_col

    def own_half(array):
        return jnp.where(core == 0, array[:half], array[half:])

    other_sides = from_mask(sides, 1)
    share = own_half(jnp.where(mine[0], sides[0], other_sides[0]))
    arrived = to_all(share, "row", peers)

    chip = lax.shift_right_logical(owner[-1], jnp.int32(1))
    head = jnp.stack([me, core, chip])
    at = jnp.concatenate([head, place, mine.astype(jnp.int32)]).astype(jnp.int32)
    *own_rows, inverses = window_rows(at, factor, diag_inverse)
    other_rows = [from_mask(rows, 1) for rows in own_rows]
    masks = owner[1:] ^ owner[:-1]
    parts = [
        [
            lax.shift_right_logical(masks[section], jnp.int32(low)) & ((1 << bits) - 1)
            for low, bits in levels(cols)
        ]
        for section in range(section_count - 1)
    ]
    live = order[:, None] < live_segments[None, :]
    taken = (here & mine[:, None])[:, None, :] & live[:, :, None]
    done = taken.any(axis=0)[:, :, None]
    first = (arrived, parts, at, live, taken, done, sides, other_sides, own_rows, other_rows, inverses)
    arrived, parts, at, live, taken, done, sides, other_sides, own_rows, other_rows, inverses = (
        lax.optimization_barrier(first)
    )

    remaining = jnp.moveaxis(arrived, 0, 1).reshape(half, tile_width)
    history = None
    result = jnp.zeros_like(right_side)
    for section in range(section_count):
        if section:
            copies = partial_half(
                section,
                at,
                history,
                own_rows[section - 1],
                other_rows[section - 1],
                sides,
                other_sides,
                peers,
            )
            copies, history, result = lax.optimization_barrier((copies, history, result))
            remaining = lax.all_to_all(copies, "row", 0, 0, tiled=True).sum(axis=0)
        solved = lax.dot_general(
            remaining,
            inverses[section].astype(F32),
            NT,
            precision=lax.Precision.HIGHEST,
            preferred_element_type=F32,
        )
        other = from_mask(solved, 1)
        solved = jnp.where(
            core == 0, jnp.concatenate([solved, other]), jnp.concatenate([other, solved])
        )
        result = jnp.where(taken[section][..., None], solved[:, None, :], result)
        sent = jnp.where(live[section][:, None], solved, 0.0).astype(BF16)[None]
        history = sent if history is None else jnp.concatenate([history, sent])
        if section < section_count - 1:
            history, result = lax.optimization_barrier((history, result))
            history = moved_by_mask(history, parts[section])
    history, result = lax.optimization_barrier((history, result))
    planes = [list(range(first, cols, 2)) for first in range(2)]
    everywhere = to_all(history, "col", cols // 2, planes)
    pieces = trailing(at, everywhere, factor, tile_width, peers)
    total = lax.all_to_all(pieces, "row", 0, 0, tiled=True).sum(axis=0)
    updated = right_side - jnp.moveaxis(total, 0, 1)
    return jnp.where(done, result, updated)


def solution(mesh):
    return jax.shard_map(
        per_device,
        mesh=mesh,
        in_specs=(P("col", None, "row"), P(None, "row", None), P(None, "col", "row"), P(), P()),
        out_specs=P(None, "col", "row"),
        check_vma=False,
    )
```

```python
import functools

import jax
import jax.numpy as jnp
from jax import lax
from jax.experimental import pallas as pl
from jax.experimental.pallas import tpu as pltpu
from jax.sharding import PartitionSpec as P


NT = (((1,), (1,)), ((), ()))
F32 = jnp.float32
BF16 = jnp.bfloat16
CHIP, PLACE, MINE = 2, 3, 8


def to_all(array, axis, peers, groups=None):
    copies = jnp.broadcast_to(array[None], (peers, *array.shape))
    return lax.all_to_all(copies, axis, 0, 0, axis_index_groups=groups, tiled=True)


def from_mask(array, mask):
    size = lax.axis_size("col")
    return lax.ppermute(array, "col", [(i, i ^ mask) for i in range(size)])


def levels(size):
    bits = size.bit_length() - 1
    return [(low, min(2, bits - low)) for low in range(1, bits, 2)][::-1]


def moved_by_mask(array, parts):
    for (low, bits), part in zip(levels(lax.axis_size("col")), parts, strict=True):
        branches = [lambda value: value]
        for step in range(1, 1 << bits):
            branches.append(functools.partial(from_mask, mask=step << low))
        array = lax.switch(part, branches, array)
    return array


def window_kernel(at_ref, factor_ref, diag_ref, *refs):
    *row_refs, inverse_ref, sems = refs
    tile_width = row_refs[0].shape[1]
    copies = []
    for t, out_ref in enumerate(row_refs, 1):
        start = pl.multiple_of(at_ref[PLACE + t] * tile_width, tile_width)
        rows = factor_ref.at[pl.ds(0, t), pl.ds(start, tile_width), :]
        copies.append(pltpu.make_async_copy(rows, out_ref, sems.at[t]))
    copies.append(pltpu.make_async_copy(diag_ref.at[0], inverse_ref, sems.at[0]))
    for copy in copies:
        copy.start()
    for copy in copies:
        copy.wait()


def window_rows(at, factor, diag_inverse):
    section_count, width, tile_width = diag_inverse.shape
    shapes = [(t, tile_width, width) for t in range(1, section_count)] + [(width, tile_width)]
    in_place = pl.BlockSpec(memory_space=pltpu.HBM)
    return pl.pallas_call(
        window_kernel,
        out_shape=[jax.ShapeDtypeStruct(shape, factor.dtype) for shape in shapes],
        grid_spec=pltpu.PrefetchScalarGridSpec(
            num_scalar_prefetch=1,
            grid=(1,),
            in_specs=[in_place, in_place],
            out_specs=[
                pl.BlockSpec(shape, lambda i, at, rank=len(shape): (0,) * rank) for shape in shapes
            ],
            scratch_shapes=[pltpu.SemaphoreType.DMA((section_count,))],
        ),
        compiler_params=pltpu.CompilerParams(vmem_limit_bytes=8 << 20),
        cost_estimate=pl.CostEstimate(flops=0, bytes_accessed=5 << 20, transcendentals=0),
    )(at, factor, diag_inverse)


def partial_kernel(
    section, at_ref, sent_ref, own_ref, other_ref, own_side, other_side, diag_ref, out_ref, inverse_ref
):
    inverse_ref[...] = diag_ref[0]
    me, core = at_ref[0], at_ref[1]
    peers, half, _ = out_ref.shape
    width = own_side.shape[2]
    columns = pl.ds(pl.multiple_of(me * width, width), width)

    def write(rows_ref, side_ref):
        total = lax.dot_general(sent_ref[0], rows_ref[0], NT, preferred_element_type=F32)
        for before in range(1, section):
            total = total + lax.dot_general(
                sent_ref[before], rows_ref[before], NT, preferred_element_type=F32
            )
        value = -jnp.where(core == 0, total[:half], total[half:])
        side = jnp.where(core == 0, side_ref[0, :half], side_ref[0, half:])
        for peer in range(peers):
            out_ref[peer] = value
            out_ref[peer, :, columns] = out_ref[peer, :, columns] + side

    mine = at_ref[MINE + section]

    @pl.when(mine == 1)
    def _():
        write(own_ref, own_side)

    @pl.when(mine != 1)
    def _():
        write(other_ref, other_side)


def partial_half(section, at, sent, own_rows, other_rows, own_sides, other_sides, diag_inverse, peers):
    _, rhs_count, width = sent.shape
    tile_width = own_rows.shape[1]
    half = rhs_count // 2
    rows = pl.BlockSpec((section, tile_width, width), lambda i, at: (0, 0, 0))
    side = pl.BlockSpec((1, rhs_count, width), lambda i, at: (section, 0, 0))
    return pl.pallas_call(
        functools.partial(partial_kernel, section),
        out_shape=[
            jax.ShapeDtypeStruct((peers, half, tile_width), F32),
            jax.ShapeDtypeStruct((width, tile_width), diag_inverse.dtype),
        ],
        grid_spec=pltpu.PrefetchScalarGridSpec(
            num_scalar_prefetch=1,
            grid=(1,),
            in_specs=[
                pl.BlockSpec((section, rhs_count, width), lambda i, at: (0, 0, 0)),
                rows,
                rows,
                side,
                side,
                pl.BlockSpec((1, width, tile_width), lambda i, at: (section, 0, 0)),
            ],
            out_specs=[
                pl.BlockSpec((peers, half, tile_width), lambda i, at: (0, 0, 0)),
                pl.BlockSpec((width, tile_width), lambda i, at: (0, 0)),
            ],
        ),
        compiler_params=pltpu.CompilerParams(vmem_limit_bytes=8 << 20),
        cost_estimate=pl.CostEstimate(
            flops=2 * section * rhs_count * width * tile_width,
            bytes_accessed=4 * section * width * tile_width,
            transcendentals=0,
        ),
    )(at, sent, own_rows, other_rows, own_sides, other_sides, diag_inverse)


def trailing_kernel(at_ref, sent_ref, factor_ref, out_ref, rows, sems):
    peers, tiles, _, width = out_ref.shape
    tile_width = peers * width
    copies = []
    for tile in range(tiles):
        span = pl.ds(tile * tile_width, tile_width)
        copies.append(
            pltpu.make_async_copy(factor_ref.at[:, span, :], rows.at[:, span, :], sems.at[tile])
        )
    for copy in copies:
        copy.start()
    for tile in range(tiles):
        copies[tile].wait()
        span = pl.ds(tile * tile_width, tile_width)
        total = None
        for before in range(rows.shape[0]):
            term = lax.dot_general(
                sent_ref[0, before], rows[before, span, :], NT, preferred_element_type=F32
            )
            total = term if total is None else total + term
        for peer in range(peers):
            out_ref[peer, tile] = total[:, peer * width : (peer + 1) * width]


def trailing(at, sent, factor, tile_width, peers):
    _, count, rhs_count, width = sent.shape
    tiles = factor.shape[1] // tile_width
    return pl.pallas_call(
        trailing_kernel,
        out_shape=jax.ShapeDtypeStruct((peers, tiles, rhs_count, width), F32),
        grid_spec=pltpu.PrefetchScalarGridSpec(
            num_scalar_prefetch=1,
            grid=(1,),
            in_specs=[
                pl.BlockSpec((1, count, rhs_count, width), lambda i, at: (at[CHIP], 0, 0, 0)),
                pl.BlockSpec(memory_space=pltpu.HBM),
            ],
            out_specs=pl.BlockSpec((peers, tiles, rhs_count, width), lambda i, at: (0, 0, 0, 0)),
            scratch_shapes=[
                pltpu.VMEM(factor.shape, factor.dtype),
                pltpu.SemaphoreType.DMA((tiles,)),
            ],
        ),
        compiler_params=pltpu.CompilerParams(vmem_limit_bytes=12 << 20),
        cost_estimate=pl.CostEstimate(
            flops=2 * count * rhs_count * width * tile_width * tiles,
            bytes_accessed=2 * count * width * tile_width * tiles,
            transcendentals=0,
        ),
    )(at, sent, factor)


def per_device(factor, diag_inverse, right_side, tile_order, live_segments):
    section_count, slice_width, tile_width = diag_inverse.shape
    rhs_count, rows_dev, _ = right_side.shape
    half = rhs_count // 2
    peers = tile_width // slice_width
    cols = lax.axis_size("col")
    my_col, me = lax.axis_index("col"), lax.axis_index("row")
    core = my_col & 1
    factor = jnp.transpose(factor, (1, 0, 2))
    slots = tile_order[:section_count]
    owner = lax.div(slots, jnp.int32(rows_dev))
    place = lax.rem(slots, jnp.int32(rows_dev))
    local = jnp.arange(rows_dev, dtype=jnp.int32)
    order = jnp.arange(section_count, dtype=jnp.int32)
    here = place[:, None] == local[None, :]
    sides = jnp.where(here[:, None, :, None], right_side[None], 0.0).sum(axis=2)
    mine = owner == my_col

    def own_half(array):
        return jnp.where(core == 0, array[:half], array[half:])

    other_sides = from_mask(sides, 1)
    share = own_half(jnp.where(mine[0], sides[0], other_sides[0]))
    arrived = to_all(share, "row", peers)

    chip = lax.shift_right_logical(owner[-1], jnp.int32(1))
    head = jnp.stack([me, core, chip])
    at = jnp.concatenate([head, place, mine.astype(jnp.int32)]).astype(jnp.int32)
    *own_rows, inverse = window_rows(at, factor, diag_inverse)
    other_rows = [from_mask(rows, 1) for rows in own_rows]
    masks = owner[1:] ^ owner[:-1]
    parts = [
        lax.shift_right_logical(masks, jnp.int32(low)) & ((1 << bits) - 1)
        for low, bits in levels(cols)
    ]
    live = order[:, None] < live_segments[None, :]
    taken = (here & mine[:, None])[:, None, :] & live[:, :, None]
    done = taken.any(axis=0)[:, :, None]
    first = (arrived, at, live, taken, done, sides, other_sides, own_rows, other_rows, inverse)
    arrived, at, live, taken, done, sides, other_sides, own_rows, other_rows, inverse = (
        lax.optimization_barrier(first)
    )

    remaining = jnp.moveaxis(arrived, 0, 1).reshape(half, tile_width)
    history = None
    result = jnp.zeros_like(right_side)
    for section in range(section_count):
        if section:
            copies, inverse = partial_half(
                section,
                at,
                history,
                own_rows[section - 1],
                other_rows[section - 1],
                sides,
                other_sides,
                diag_inverse,
                peers,
            )
            copies, inverse, history, result = lax.optimization_barrier(
                (copies, inverse, history, result)
            )
            remaining = lax.all_to_all(copies, "row", 0, 0, tiled=True).sum(axis=0)
        solved = lax.dot_general(
            remaining,
            inverse.astype(F32),
            NT,
            precision=lax.Precision.HIGHEST,
            preferred_element_type=F32,
        )
        other = from_mask(solved, 1)
        solved = jnp.where(
            core == 0, jnp.concatenate([solved, other]), jnp.concatenate([other, solved])
        )
        result = jnp.where(taken[section][..., None], solved[:, None, :], result)
        sent = jnp.where(live[section][:, None], solved, 0.0).astype(BF16)[None]
        history = sent if history is None else jnp.concatenate([history, sent])
        if section < section_count - 1:
            history, result = lax.optimization_barrier((history, result))
            history = moved_by_mask(history, [part[section] for part in parts])
    history, result = lax.optimization_barrier((history, result))
    planes = [list(range(first, cols, 2)) for first in range(2)]
    everywhere = to_all(history, "col", cols // 2, planes)
    pieces = trailing(at, everywhere, factor, tile_width, peers)
    total = lax.all_to_all(pieces, "row", 0, 0, tiled=True).sum(axis=0)
    updated = right_side - jnp.moveaxis(total, 0, 1)
    return jnp.where(done, result, updated)


def solution(mesh):
    return jax.shard_map(
        per_device,
        mesh=mesh,
        in_specs=(P("col", None, "row"), P(None, "row", None), P(None, "col", "row"), P(), P()),
        out_specs=P(None, "col", "row"),
        check_vma=False,
    )
```

```python
import functools

import jax
import jax.numpy as jnp
from jax import lax
from jax.experimental import pallas as pl
from jax.experimental.pallas import tpu as pltpu
from jax.sharding import PartitionSpec as P


NT = (((1,), (1,)), ((), ()))
F32 = jnp.float32
BF16 = jnp.bfloat16
CHIP, PLACE, MINE = 2, 3, 8


def to_all(array, axis, peers, groups=None):
    copies = jnp.broadcast_to(array[None], (peers, *array.shape))
    return lax.all_to_all(copies, axis, 0, 0, axis_index_groups=groups, tiled=True)


def from_mask(array, mask):
    size = lax.axis_size("col")
    return lax.ppermute(array, "col", [(i, i ^ mask) for i in range(size)])


def levels(size):
    bits = size.bit_length() - 1
    return [(low, min(2, bits - low)) for low in range(1, bits, 2)][::-1]


def moved_by_mask(array, parts):
    for (low, bits), part in zip(levels(lax.axis_size("col")), parts, strict=True):
        branches = [lambda value: value]
        for step in range(1, 1 << bits):
            branches.append(functools.partial(from_mask, mask=step << low))
        array = lax.switch(part, branches, array)
    return array


def window_kernel(at_ref, *refs):
    count = len(refs) // 2
    for rows_ref, out_ref in zip(refs[:count], refs[count:], strict=True):
        out_ref[...] = rows_ref[...]


def window_rows(at, factor, section_count, tile_width):
    width = factor.shape[2]

    def spec(section, index_map):
        return pl.BlockSpec((section, tile_width, width), index_map)

    later = range(1, section_count)
    return pl.pallas_call(
        window_kernel,
        out_shape=[jax.ShapeDtypeStruct((t, tile_width, width), factor.dtype) for t in later],
        grid_spec=pltpu.PrefetchScalarGridSpec(
            num_scalar_prefetch=1,
            grid=(1,),
            in_specs=[spec(t, lambda i, at, t=t: (0, at[PLACE + t], 0)) for t in later],
            out_specs=[spec(t, lambda i, at: (0, 0, 0)) for t in later],
        ),
        compiler_params=pltpu.CompilerParams(vmem_limit_bytes=14 << 20),
        cost_estimate=pl.CostEstimate(flops=0, bytes_accessed=5 << 20, transcendentals=0),
    )(at, *[factor for _ in later])


def partial_kernel(section, at_ref, sent_ref, own_ref, other_ref, own_side, other_side, out_ref):
    me, core = at_ref[0], at_ref[1]
    peers, half, _ = out_ref.shape
    width = own_side.shape[2]
    columns = pl.ds(pl.multiple_of(me * width, width), width)

    def write(rows_ref, side_ref):
        total = lax.dot_general(sent_ref[0], rows_ref[0], NT, preferred_element_type=F32)
        for before in range(1, section):
            total = total + lax.dot_general(
                sent_ref[before], rows_ref[before], NT, preferred_element_type=F32
            )
        value = -jnp.where(core == 0, total[:half], total[half:])
        side = jnp.where(core == 0, side_ref[0, :half], side_ref[0, half:])
        for peer in range(peers):
            out_ref[peer] = value
            out_ref[peer, :, columns] = out_ref[peer, :, columns] + side

    mine = at_ref[MINE + section]

    @pl.when(mine == 1)
    def _():
        write(own_ref, own_side)

    @pl.when(mine != 1)
    def _():
        write(other_ref, other_side)


def partial_half(section, at, sent, own_rows, other_rows, own_sides, other_sides, peers):
    _, rhs_count, width = sent.shape
    tile_width = own_rows.shape[1]
    half = rhs_count // 2
    rows = pl.BlockSpec((section, tile_width, width), lambda i, at: (0, 0, 0))
    side = pl.BlockSpec((1, rhs_count, width), lambda i, at: (section, 0, 0))
    return pl.pallas_call(
        functools.partial(partial_kernel, section),
        out_shape=jax.ShapeDtypeStruct((peers, half, tile_width), F32),
        grid_spec=pltpu.PrefetchScalarGridSpec(
            num_scalar_prefetch=1,
            grid=(1,),
            in_specs=[
                pl.BlockSpec((section, rhs_count, width), lambda i, at: (0, 0, 0)),
                rows,
                rows,
                side,
                side,
            ],
            out_specs=pl.BlockSpec((peers, half, tile_width), lambda i, at: (0, 0, 0)),
        ),
        compiler_params=pltpu.CompilerParams(vmem_limit_bytes=8 << 20),
        cost_estimate=pl.CostEstimate(
            flops=2 * section * rhs_count * width * tile_width,
            bytes_accessed=4 * section * width * tile_width,
            transcendentals=0,
        ),
    )(at, sent, own_rows, other_rows, own_sides, other_sides)


def trailing_kernel(at_ref, sent_ref, rows_ref, out_ref):
    total = lax.dot_general(sent_ref[0, 0], rows_ref[0], NT, preferred_element_type=F32)
    for before in range(1, rows_ref.shape[0]):
        total = total + lax.dot_general(
            sent_ref[0, before], rows_ref[before], NT, preferred_element_type=F32
        )
    width = out_ref.shape[3]
    for peer in range(out_ref.shape[0]):
        out_ref[peer, 0] = total[:, peer * width : (peer + 1) * width]


def trailing(at, sent, factor, tile_width, peers):
    _, count, rhs_count, width = sent.shape
    tiles = factor.shape[1] // tile_width
    return pl.pallas_call(
        trailing_kernel,
        out_shape=jax.ShapeDtypeStruct((peers, tiles, rhs_count, width), F32),
        grid_spec=pltpu.PrefetchScalarGridSpec(
            num_scalar_prefetch=1,
            grid=(tiles,),
            in_specs=[
                pl.BlockSpec((1, count, rhs_count, width), lambda i, at: (at[CHIP], 0, 0, 0)),
                pl.BlockSpec((count, tile_width, width), lambda i, at: (0, i, 0)),
            ],
            out_specs=pl.BlockSpec((peers, 1, rhs_count, width), lambda i, at: (0, i, 0, 0)),
        ),
        compiler_params=pltpu.CompilerParams(vmem_limit_bytes=10 << 20),
        cost_estimate=pl.CostEstimate(
            flops=2 * count * rhs_count * width * tile_width * tiles,
            bytes_accessed=2 * count * width * tile_width * tiles,
            transcendentals=0,
        ),
    )(at, sent, factor)


def per_device(factor, diag_inverse, right_side, tile_order, live_segments):
    section_count, slice_width, tile_width = diag_inverse.shape
    rhs_count, rows_dev, _ = right_side.shape
    half = rhs_count // 2
    peers = tile_width // slice_width
    cols = lax.axis_size("col")
    my_col, me = lax.axis_index("col"), lax.axis_index("row")
    core = my_col & 1
    factor = jnp.transpose(factor, (1, 0, 2))
    slots = tile_order[:section_count]
    owner = lax.div(slots, jnp.int32(rows_dev))
    place = lax.rem(slots, jnp.int32(rows_dev))
    local = jnp.arange(rows_dev, dtype=jnp.int32)
    order = jnp.arange(section_count, dtype=jnp.int32)
    here = place[:, None] == local[None, :]
    sides = jnp.where(here[:, None, :, None], right_side[None], 0.0).sum(axis=2)
    mine = owner == my_col

    def own_half(array):
        return jnp.where(core == 0, array[:half], array[half:])

    other_sides = from_mask(sides, 1)
    share = own_half(jnp.where(mine[0], sides[0], other_sides[0]))
    arrived = to_all(share, "row", peers)

    chip = lax.shift_right_logical(owner[-1], jnp.int32(1))
    head = jnp.stack([me, core, chip])
    at = jnp.concatenate([head, place, mine.astype(jnp.int32)]).astype(jnp.int32)
    own_rows = window_rows(at, factor, section_count, tile_width)
    other_rows = [from_mask(rows, 1) for rows in own_rows]
    masks = owner[1:] ^ owner[:-1]
    parts = [
        lax.shift_right_logical(masks, jnp.int32(low)) & ((1 << bits) - 1)
        for low, bits in levels(cols)
    ]
    live = order[:, None] < live_segments[None, :]
    taken = (here & mine[:, None])[:, None, :] & live[:, :, None]
    done = taken.any(axis=0)[:, :, None]
    first = (arrived, at, live, taken, done, sides, other_sides, own_rows, other_rows)
    arrived, at, live, taken, done, sides, other_sides, own_rows, other_rows = (
        lax.optimization_barrier(first)
    )

    remaining = jnp.moveaxis(arrived, 0, 1).reshape(half, tile_width)
    history = None
    solves = []
    for section in range(section_count):
        if section:
            copies = partial_half(
                section,
                at,
                history,
                own_rows[section - 1],
                other_rows[section - 1],
                sides,
                other_sides,
                peers,
            )
            copies, history, solves = lax.optimization_barrier((copies, history, solves))
            remaining = lax.all_to_all(copies, "row", 0, 0, tiled=True).sum(axis=0)
        solved = lax.dot_general(
            remaining,
            diag_inverse[section].astype(F32),
            NT,
            precision=lax.Precision.HIGHEST,
            preferred_element_type=F32,
        )
        other = from_mask(solved, 1)
        solved = jnp.where(
            core == 0, jnp.concatenate([solved, other]), jnp.concatenate([other, solved])
        )
        solves.append(solved)
        sent = jnp.where(live[section][:, None], solved, 0.0).astype(BF16)[None]
        history = sent if history is None else jnp.concatenate([history, sent])
        if section < section_count - 1:
            history, solves = lax.optimization_barrier((history, solves))
            history = moved_by_mask(history, [part[section] for part in parts])
    result = jnp.where(taken[..., None], jnp.stack(solves)[:, :, None, :], 0.0).sum(axis=0)
    history, result = lax.optimization_barrier((history, result))
    planes = [list(range(first, cols, 2)) for first in range(2)]
    everywhere = to_all(history, "col", cols // 2, planes)
    pieces = trailing(at, everywhere, factor, tile_width, peers)
    total = lax.all_to_all(pieces, "row", 0, 0, tiled=True).sum(axis=0)
    updated = right_side - jnp.moveaxis(total, 0, 1)
    return jnp.where(done, result, updated)


def solution(mesh):
    return jax.shard_map(
        per_device,
        mesh=mesh,
        in_specs=(P("col", None, "row"), P(None, "row", None), P(None, "col", "row"), P(), P()),
        out_specs=P(None, "col", "row"),
        check_vma=False,
    )
```

```python
import functools

import jax
import jax.numpy as jnp
from jax import lax
from jax.experimental import pallas as pl
from jax.experimental.pallas import tpu as pltpu
from jax.sharding import PartitionSpec as P


NT = (((1,), (1,)), ((), ()))
F32 = jnp.float32
BF16 = jnp.bfloat16
CHIP, PLACE, MINE = 2, 3, 8


def to_all(array, axis, peers, groups=None):
    copies = jnp.broadcast_to(array[None], (peers, *array.shape))
    return lax.all_to_all(copies, axis, 0, 0, axis_index_groups=groups, tiled=True)


def from_mask(array, mask):
    size = lax.axis_size("col")
    return lax.ppermute(array, "col", [(i, i ^ mask) for i in range(size)])


def levels(size):
    bits = size.bit_length() - 1
    return [(low, min(2, bits - low)) for low in range(1, bits, 2)][::-1]


def moved_by_mask(array, parts):
    for (low, bits), part in zip(levels(lax.axis_size("col")), parts, strict=True):
        branches = [lambda value: value]
        for step in range(1, 1 << bits):
            branches.append(functools.partial(from_mask, mask=step << low))
        array = lax.switch(part, branches, array)
    return array


def window_kernel(at_ref, *refs):
    count = len(refs) // 2
    for rows_ref, out_ref in zip(refs[:count], refs[count:], strict=True):
        out_ref[...] = rows_ref[...]


def window_rows(at, factor, section_count, tile_width):
    width = factor.shape[2]

    def spec(section, index_map):
        return pl.BlockSpec((section, tile_width, width), index_map)

    later = range(1, section_count)
    return pl.pallas_call(
        window_kernel,
        out_shape=[jax.ShapeDtypeStruct((t, tile_width, width), factor.dtype) for t in later],
        grid_spec=pltpu.PrefetchScalarGridSpec(
            num_scalar_prefetch=1,
            grid=(1,),
            in_specs=[spec(t, lambda i, at, t=t: (0, at[PLACE + t], 0)) for t in later],
            out_specs=[spec(t, lambda i, at: (0, 0, 0)) for t in later],
        ),
        compiler_params=pltpu.CompilerParams(vmem_limit_bytes=14 << 20),
        cost_estimate=pl.CostEstimate(flops=0, bytes_accessed=5 << 20, transcendentals=0),
    )(at, *[factor for _ in later])


def partial_kernel(section, at_ref, sent_ref, own_ref, other_ref, own_side, other_side, out_ref):
    me, core = at_ref[0], at_ref[1]
    peers, half, _ = out_ref.shape
    width = own_side.shape[2]
    columns = pl.ds(pl.multiple_of(me * width, width), width)

    def write(rows_ref, side_ref):
        total = lax.dot_general(sent_ref[0], rows_ref[0], NT, preferred_element_type=F32)
        for before in range(1, section):
            total = total + lax.dot_general(
                sent_ref[before], rows_ref[before], NT, preferred_element_type=F32
            )
        value = -jnp.where(core == 0, total[:half], total[half:])
        side = jnp.where(core == 0, side_ref[0, :half], side_ref[0, half:])
        for peer in range(peers):
            out_ref[peer] = value
            out_ref[peer, :, columns] = out_ref[peer, :, columns] + side

    mine = at_ref[MINE + section]

    @pl.when(mine == 1)
    def _():
        write(own_ref, own_side)

    @pl.when(mine != 1)
    def _():
        write(other_ref, other_side)


def partial_half(section, at, sent, own_rows, other_rows, own_sides, other_sides, peers):
    _, rhs_count, width = sent.shape
    tile_width = own_rows.shape[1]
    half = rhs_count // 2
    rows = pl.BlockSpec((section, tile_width, width), lambda i, at: (0, 0, 0))
    side = pl.BlockSpec((1, rhs_count, width), lambda i, at: (section, 0, 0))
    return pl.pallas_call(
        functools.partial(partial_kernel, section),
        out_shape=jax.ShapeDtypeStruct((peers, half, tile_width), F32),
        grid_spec=pltpu.PrefetchScalarGridSpec(
            num_scalar_prefetch=1,
            grid=(1,),
            in_specs=[
                pl.BlockSpec((section, rhs_count, width), lambda i, at: (0, 0, 0)),
                rows,
                rows,
                side,
                side,
            ],
            out_specs=pl.BlockSpec((peers, half, tile_width), lambda i, at: (0, 0, 0)),
        ),
        compiler_params=pltpu.CompilerParams(vmem_limit_bytes=8 << 20),
        cost_estimate=pl.CostEstimate(
            flops=2 * section * rhs_count * width * tile_width,
            bytes_accessed=4 * section * width * tile_width,
            transcendentals=0,
        ),
    )(at, sent, own_rows, other_rows, own_sides, other_sides)


def trailing_kernel(at_ref, sent_ref, rows_ref, out_ref):
    total = lax.dot_general(sent_ref[0, 0], rows_ref[0], NT, preferred_element_type=F32)
    for before in range(1, rows_ref.shape[0]):
        total = total + lax.dot_general(
            sent_ref[0, before], rows_ref[before], NT, preferred_element_type=F32
        )
    width = out_ref.shape[3]
    for peer in range(out_ref.shape[0]):
        out_ref[peer, 0] = total[:, peer * width : (peer + 1) * width]


def trailing(at, sent, factor, tile_width, peers):
    _, count, rhs_count, width = sent.shape
    tiles = factor.shape[1] // tile_width
    return pl.pallas_call(
        trailing_kernel,
        out_shape=jax.ShapeDtypeStruct((peers, tiles, rhs_count, width), F32),
        grid_spec=pltpu.PrefetchScalarGridSpec(
            num_scalar_prefetch=1,
            grid=(tiles,),
            in_specs=[
                pl.BlockSpec((1, count, rhs_count, width), lambda i, at: (at[CHIP], 0, 0, 0)),
                pl.BlockSpec((count, tile_width, width), lambda i, at: (0, i, 0)),
            ],
            out_specs=pl.BlockSpec((peers, 1, rhs_count, width), lambda i, at: (0, i, 0, 0)),
        ),
        compiler_params=pltpu.CompilerParams(vmem_limit_bytes=10 << 20),
        cost_estimate=pl.CostEstimate(
            flops=2 * count * rhs_count * width * tile_width * tiles,
            bytes_accessed=2 * count * width * tile_width * tiles,
            transcendentals=0,
        ),
    )(at, sent, factor)


def per_device(factor, diag_inverse, right_side, tile_order, live_segments):
    section_count, slice_width, tile_width = diag_inverse.shape
    rhs_count, rows_dev, _ = right_side.shape
    half = rhs_count // 2
    peers = tile_width // slice_width
    cols = lax.axis_size("col")
    my_col, me = lax.axis_index("col"), lax.axis_index("row")
    core = my_col & 1
    factor = jnp.transpose(factor, (1, 0, 2))
    slots = tile_order[:section_count]
    owner = lax.div(slots, jnp.int32(rows_dev))
    place = lax.rem(slots, jnp.int32(rows_dev))
    local = jnp.arange(rows_dev, dtype=jnp.int32)
    order = jnp.arange(section_count, dtype=jnp.int32)
    here = place[:, None] == local[None, :]
    sides = jnp.where(here[:, None, :, None], right_side[None], 0.0).sum(axis=2)
    mine = owner == my_col

    def own_half(array):
        return jnp.where(core == 0, array[:half], array[half:])

    other_sides = from_mask(sides, 1)
    share = own_half(jnp.where(mine[:, None, None], sides, other_sides)[0])
    arrived = to_all(share, "row", peers)

    chip = lax.shift_right_logical(owner[-1], jnp.int32(1))
    head = jnp.stack([me, core, chip])
    at = jnp.concatenate([head, place, mine.astype(jnp.int32)]).astype(jnp.int32)
    own_rows = window_rows(at, factor, section_count, tile_width)
    other_rows = [from_mask(rows, 1) for rows in own_rows]
    masks = owner[1:] ^ owner[:-1]
    parts = [
        lax.shift_right_logical(masks, jnp.int32(low)) & ((1 << bits) - 1)
        for low, bits in levels(cols)
    ]
    live = order[:, None] < live_segments[None, :]
    taken = (here & mine[:, None])[:, None, :] & live[:, :, None]
    live = jnp.broadcast_to(live[:, :, None].astype(F32), sides.shape)
    done = taken.any(axis=0)[:, :, None]
    first = (arrived, at, live, taken, done, sides, other_sides, own_rows, other_rows)
    arrived, at, live, taken, done, sides, other_sides, own_rows, other_rows = (
        lax.optimization_barrier(first)
    )

    remaining = jnp.moveaxis(arrived, 0, 1).reshape(half, tile_width)
    history = None
    solves = []
    for section in range(section_count):
        if section:
            copies = partial_half(
                section,
                at,
                history,
                own_rows[section - 1],
                other_rows[section - 1],
                sides,
                other_sides,
                peers,
            )
            copies, history, solves = lax.optimization_barrier((copies, history, solves))
            remaining = lax.all_to_all(copies, "row", 0, 0, tiled=True).sum(axis=0)
        solved = lax.dot_general(
            remaining,
            diag_inverse[section].astype(F32),
            NT,
            precision=lax.Precision.HIGHEST,
            preferred_element_type=F32,
        )
        other = from_mask(solved, 1)
        solved = jnp.where(
            core == 0, jnp.concatenate([solved, other]), jnp.concatenate([other, solved])
        )
        solves.append(solved)
        sent = jnp.where(live[section] > 0, solved, 0.0).astype(BF16)[None]
        history = sent if history is None else jnp.concatenate([history, sent])
        if section < section_count - 1:
            history, solves = lax.optimization_barrier((history, solves))
            history = moved_by_mask(history, [part[section] for part in parts])
    result = jnp.where(taken[..., None], jnp.stack(solves)[:, :, None, :], 0.0).sum(axis=0)
    history, result = lax.optimization_barrier((history, result))
    planes = [list(range(first, cols, 2)) for first in range(2)]
    everywhere = to_all(history, "col", cols // 2, planes)
    pieces = trailing(at, everywhere, factor, tile_width, peers)
    total = lax.all_to_all(pieces, "row", 0, 0, tiled=True).sum(axis=0)
    updated = right_side - jnp.moveaxis(total, 0, 1)
    return jnp.where(done, result, updated)


def solution(mesh):
    return jax.shard_map(
        per_device,
        mesh=mesh,
        in_specs=(P("col", None, "row"), P(None, "row", None), P(None, "col", "row"), P(), P()),
        out_specs=P(None, "col", "row"),
        check_vma=False,
    )
```
